512 devices in a mesh: row: 16 (over x, y), col: 32 (over z, core).
Axes of the slice: x: 4, y: 4, z: 16, core: 2. Of those that a mesh axis runs over, the one named last changes fastest.
Arguments:
- arrival: float32 [64, 16384], P(None, 'col'), may hold values from 0 to 4
- delay: bfloat16 [4, 16384, 16384], P(None, 'col', 'row'), may hold values from -40 to 20
- occupancy: int32 [4, 32, 32], replicated, may hold values from 0 to 1, as said below
Outputs:
- final_arrival: float32 [64, 16384], P(None, 'col')
- worst: float32 [64], replicated
The draws below stay inside these ranges and needn't reach their ends.
Inputs may be any that keep to these rules, and one draw needn't show every extreme that they name: In every level every column of tiles holds at least one tile with occupancy 1.
All inputs are finite; a program needn't handle non-finite values.
Results may differ from the reference program's by a relative error of at most 0.0009.
Values sent between devices are 32-bit elements; how exact they have to be, the bound alone decides.
A program may use at most 64 MiB of HBM per device.

```python
import jax
import jax.numpy as jnp
from jax import lax

TILE = 512
SCEN = 64
LEVELS = 4
TILES = 32
PINS = 16384


def draw_occupancy(key, part):
    first, second = jax.random.split(jax.random.fold_in(key, 7))
    base = jax.random.randint(first, (LEVELS, TILES, TILES), 0, 2, dtype=jnp.int32)
    picked = jax.random.randint(second, (LEVELS, 1, TILES), 0, TILES, dtype=jnp.int32)
    places = jnp.arange(TILES, dtype=jnp.int32)[None, :, None]
    forced = (places == picked).astype(jnp.int32)
    return jnp.maximum(base, forced)


def draw_delay(key, part):
    spread = jnp.float32(2.5)
    nominal = spread * jnp.sqrt(2.0 * jnp.log(jnp.float32(0.5 * PINS)))
    first, second, third = jax.random.split(jax.random.fold_in(key, 11), 3)
    normal_part = jnp.clip(jax.random.normal(first, (LEVELS, PINS, PINS), jnp.float32), -6.0, 6.0)
    values = spread * normal_part - nominal
    return jnp.clip(values, -40.0, 20.0).astype(jnp.bfloat16)


def levels(rng, shape, pieces, smallest, high):
    level, own = 1.0, jax.random.fold_in(rng, 6)
    for dim, parts in pieces:
        heights = jnp.exp(jax.random.uniform(jax.random.fold_in(own, dim), (parts,), jnp.float32, smallest / len(pieces), high / len(pieces)))
        level = level * jnp.repeat(heights, shape[dim] // parts).reshape([-1 if axis == dim else 1 for axis in range(len(shape))])
    return level


def setup_inputs(seed: int = 0) -> dict:
    key_list = jax.random.split(jax.random.key(seed), 4)
    return {
        "arrival": jnp.clip(4.0 * jax.random.uniform(key_list[0], (SCEN, PINS), jnp.float32) ** levels(key_list[0], (SCEN, PINS), ((1, 32),), -0.2, 0.2), 0.0, 4.0),
        "delay": draw_delay(jax.random.fold_in(key_list[3], 71), 0),
        "occupancy": draw_occupancy(jax.random.fold_in(key_list[3], 71), 0),
    }


def level_max(times, delay_level, flags):
    width = min(32, TILE)
    turns = PINS // width

    def step(best, index):
        start = (index * width).astype(jnp.int32)
        part_a = lax.dynamic_slice_in_dim(times, start, width, 1)
        part_d = lax.dynamic_slice_in_dim(delay_level, start, width, 0).astype(jnp.float32)
        tile_row = lax.dynamic_index_in_dim(flags, (start // TILE).astype(jnp.int32), 0, keepdims=False)
        keep = jnp.repeat(tile_row > 0, TILE)
        masked = jnp.where(keep[None, :], part_d, jnp.float32(-1e9))
        return jnp.maximum(best, jnp.max(part_a[:, :, None] + masked[None, :, :], axis=1)), None

    init = jnp.full((times.shape[0], PINS), -1e9, jnp.float32)
    best, unused = lax.scan(step, init, jnp.arange(turns, dtype=jnp.int32))
    return best


def reference(arrival, delay, occupancy):
    times = arrival
    for level in range(LEVELS):
        times = level_max(times, delay[level], occupancy[level])
    return times, jnp.max(times, axis=1)
```

```python
import functools

import jax
import jax.numpy as jnp
from jax import lax
from jax.experimental import pallas as pl
from jax.experimental.pallas import tpu as pltpu
from jax.sharding import PartitionSpec as P

MESH = pl.DeviceIdType.MESH
LANES = 128
GROUPS = 4
LOW = -1000000000.0


def kernel(
    rows, cols, arrival_ref, delay_hbm, occ_ref, out_ref, worst_ref,
    delay_ref, wide_ref, times_ref, part_ref, near_ref, comb_ref, far_ref, fin_ref, crest_ref, peak_ref, top_ref,
    load_sem, near_send, near_recv, far_send, far_recv, times_send, times_recv, peak_send, peak_recv, top_send, top_recv,
):
    level_count, tile, width = delay_hbm.shape
    groups, side, gscen, sp = times_ref.shape[1:]
    ratio = cols // rows
    row = lax.axis_index("row")
    col = lax.axis_index("col")
    x = row // side
    y = row % side
    z = col // ratio
    p = col % ratio
    keeper = z % side == y
    last = level_count - 1

    def turn(value, n, size):
        return lax.rem(value + n, size)

    barrier = pltpu.get_barrier_semaphore()

    def greet(to_row, to_col):
        pl.semaphore_signal(barrier, inc=1, device_id=(to_row, to_col), device_id_type=MESH)

    for n in range(1, cols):
        greet(row, turn(col, n, cols))
    for n in range(1, rows):
        greet(turn(row, n, rows), col)
    for i in range(1, side):
        for c in range(1, ratio):
            greet(turn(x, i, side) * side + y, z * ratio + turn(p, c, ratio))
    peers = cols - 1 + rows - 1 + (side - 1) * (ratio - 1)

    def load(level):
        return pltpu.make_async_copy(delay_hbm.at[level], delay_ref.at[level], load_sem.at[level])

    for level in range(level_count):
        load(level).start()

    def widen(level):
        def step(i, carry):
            at = pl.ds(pl.multiple_of(i * 64, 64), 64)
            wide_ref[level, pl.ds(i * 8, 8)] = delay_ref[level, at, :].astype(jnp.float32).reshape(8, 8, width)
            return carry

        lax.fori_loop(0, tile // 64, step, 0)

    for g in range(groups):
        for k in range(side):
            times_ref[0, g, k] = arrival_ref[g * gscen:(g + 1) * gscen, k * sp:(k + 1) * sp]
    load(0).wait()
    widen(0)
    pl.semaphore_wait(barrier, peers)

    def near_copy(level, g, i, c):
        to_x = turn(x, i, side)
        to_p = turn(p, c, ratio)
        return pltpu.make_async_remote_copy(
            src_ref=part_ref.at[level, g, to_p * side + to_x], dst_ref=near_ref.at[level, g, i * ratio + c],
            send_sem=near_send.at[level, g], recv_sem=near_recv.at[level, g],
            device_id=(to_x * side + y, z * ratio + to_p), device_id_type=MESH)

    def near_all(level, g):
        some = near_ref.at[level, g, pl.ds(1, side * ratio - 1)]
        return pltpu.make_async_remote_copy(
            src_ref=some, dst_ref=some, send_sem=near_send.at[level, g], recv_sem=near_recv.at[level, g],
            device_id=(turn(x, 1, side) * side + y, col), device_id_type=MESH)

    def spot(i):
        return turn(x, side - i, side) * side + y

    def far_copy(level, g, i):
        return pltpu.make_async_remote_copy(
            src_ref=comb_ref.at[level, g, i], dst_ref=far_ref.at[level, g, turn(z, rows - spot(i), rows)],
            send_sem=far_send.at[level, g], recv_sem=far_recv.at[level, g],
            device_id=(row, spot(i) * ratio + p), device_id_type=MESH)

    def far_all(level, g, count):
        some = far_ref.at[level, g, pl.ds(1, count)]
        return pltpu.make_async_remote_copy(
            src_ref=some, dst_ref=some, send_sem=far_send.at[level, g], recv_sem=far_recv.at[level, g],
            device_id=(row, turn(z, 1, rows) * ratio + p), device_id_type=MESH)

    steps = sorted(
        ((a, b) for a in range(side) for b in range(side) if a or b),
        key=lambda s: -(min(s[0], side - s[0]) + min(s[1], side - s[1])))

    def times_copy(level, g, a, b, k):
        return pltpu.make_async_remote_copy(
            src_ref=fin_ref.at[level, g], dst_ref=times_ref.at[level + 1, g, k],
            send_sem=times_send.at[level, g], recv_sem=times_recv.at[level, g, k],
            device_id=(turn(x, a, side) * side + turn(y, b, side), col), device_id_type=MESH)

    def times_all(level, g):
        some = far_ref.at[level, g, pl.ds(1, rows - 1)]
        return pltpu.make_async_remote_copy(
            src_ref=some, dst_ref=some, send_sem=times_send.at[level, g], recv_sem=times_recv.at[level, g, 0],
            device_id=(turn(row, 1, rows), col), device_id_type=MESH)

    def wait_times(level, g, k):
        @pl.when(jnp.logical_not(jnp.logical_and(keeper, k == x)))
        def _():
            times_copy(level, g, 0, 1, k).wait_recv()

    def compute(level, g, hooks):
        def step(n, best):
            for at, hook in hooks:
                pl.when(n == at)(hook)
            k = turn(x, jnp.where(n < 2, n, side + 1 - n), side)

            @pl.when(level > 0)
            def _():
                wait_times(level - 1, g, k)

            value = times_ref[level, g, k]
            for i in range(sp):
                spread = jnp.broadcast_to(value[:, i:i + 1], (gscen, LANES))
                best = tuple(jnp.maximum(b, spread + wide_ref[level, k * (sp // 8) + i // 8, i % 8:i % 8 + 1, c * LANES:(c + 1) * LANES]) for c, b in enumerate(best))
            return best

        best = lax.fori_loop(0, side, step, (jnp.full((gscen, LANES), LOW, jnp.float32),) * (width // LANES))
        crest = jnp.full((gscen, LANES), LOW, jnp.float32)
        for q in range(ratio):
            flag = occ_ref[level, col, row * ratio + q]
            for k in range(side):
                piece = jnp.where(flag > 0, best[q * side + k], jnp.float32(LOW))
                part_ref[level, g, q * side + k] = piece
                crest = jnp.maximum(crest, piece)
        for i in (2, 1, 3, 0):
            for c in range(ratio):
                if i or c:
                    near_copy(level, g, i, c).start()
        crest_ref[g] = crest

    def combine(level, g):
        near_all(level, g).wait_recv()
        for i in range(side):
            total = near_ref[level, g, i * ratio] if i else part_ref[level, g, p * side + x]
            for c in range(1, ratio):
                total = jnp.maximum(total, near_ref[level, g, i * ratio + c])
            comb_ref[level, g, i] = total

            @pl.when(z != spot(i))
            def _():
                far_copy(level, g, i).start()

            @pl.when(z == spot(i))
            def _():
                far_ref[level, g, 0] = total

    def finish(level, g):
        @pl.when(keeper)
        def _():
            far_all(level, g, rows - 1).wait_recv()
            total = far_ref[level, g, 0]
            for n in range(1, rows):
                total = jnp.maximum(total, far_ref[level, g, n])
            fin_ref[level, g] = total
            for a, b in steps:
                times_copy(level, g, a, b, x).start()
            times_ref[level + 1, g, x] = total

    def settle(level):
        for g in range(groups):
            near_all(level, g).wait_send()

            @pl.when(jnp.logical_not(keeper))
            def _():
                far_all(level, g, side).wait_send()

            @pl.when(keeper)
            def _():
                far_all(level, g, side - 1).wait_send()
                times_all(level, g).wait_send()

    def peak_copy(n):
        return pltpu.make_async_remote_copy(
            src_ref=peak_ref.at[0], dst_ref=peak_ref.at[n], send_sem=peak_send.at[n], recv_sem=peak_recv.at[n],
            device_id=(row, turn(col, n, cols)), device_id_type=MESH)

    def top_copy(n):
        return pltpu.make_async_remote_copy(
            src_ref=top_ref.at[0], dst_ref=top_ref.at[n], send_sem=top_send.at[n], recv_sem=top_recv.at[n],
            device_id=(turn(row, n, rows), col), device_id_type=MESH)

    def peaks():
        lane = lax.broadcasted_iota(jnp.int32, (gscen, LANES), 1)
        line = lax.broadcasted_iota(jnp.int32, (gscen, LANES), 0)
        peak = jnp.full((1, LANES), LOW, jnp.float32)
        for g in range(groups):
            most = jnp.max(crest_ref[g], axis=1, keepdims=True)
            shown = jnp.where(lane == line + g * gscen, most, jnp.float32(LOW))
            peak = jnp.maximum(peak, jnp.max(shown, axis=0, keepdims=True))
        peak_ref[0] = peak
        for n in range(1, cols):
            peak_copy(n).start()

    def one_level(level, carry):
        @pl.when(level > 0)
        def _():
            finish(level - 1, 2)

        def late():
            @pl.when(level > 0)
            def _():
                finish(level - 1, 3)

        compute(level, 0, [(2, late)])
        compute(level, 1, [])
        compute(level, 2, [(3, lambda: combine(level, 0))])
        compute(level, 3, [(3, lambda: combine(level, 1))])

        @pl.when(level == last)
        def _():
            peaks()

        @pl.when(level < last)
        def _():
            load(level + 1).wait()
            widen(level + 1)

        combine(level, 2)

        @pl.when(level > 0)
        def _():
            settle(level - 1)

        combine(level, 3)
        finish(level, 0)
        finish(level, 1)
        return carry

    lax.fori_loop(0, level_count, one_level, 0)
    finish(last, 2)
    top = peak_ref[0]
    for n in range(1, cols):
        peak_copy(n).wait_recv()
        top = jnp.maximum(top, peak_ref[n])
    top_ref[0] = top
    for n in range(1, rows):
        top_copy(n).start()
    finish(last, 3)

    for g in range(groups):
        for k in range(side):
            wait_times(last, g, k)
            out_ref[g * gscen:(g + 1) * gscen, k * sp:(k + 1) * sp] = times_ref[level_count, g, k]
    for n in range(1, rows):
        top_copy(n).wait_recv()
        top = jnp.maximum(top, top_ref[n])
    worst_ref[...] = top
    settle(last)
    for n in range(1, cols):
        peak_copy(n).wait_send()
    for n in range(1, rows):
        top_copy(n).wait_send()


def shards(side, arrival, delay, occupancy):
    rows, cols = lax.axis_size("row"), lax.axis_size("col")
    scenarios, tile = arrival.shape
    level_count, _, width = delay.shape
    ratio = cols // rows
    sp = tile // side
    gscen = scenarios // GROUPS
    vmem = pl.BlockSpec(memory_space=pltpu.VMEM)
    f32 = jnp.float32
    dma = pltpu.SemaphoreType.DMA
    lg = (level_count, GROUPS)
    times, worst = pl.pallas_call(
        functools.partial(kernel, rows, cols),
        out_shape=(
            jax.ShapeDtypeStruct((scenarios, tile), f32),
            jax.ShapeDtypeStruct((1, LANES), f32),
        ),
        in_specs=[vmem, pl.BlockSpec(memory_space=pltpu.HBM), pl.BlockSpec(memory_space=pltpu.SMEM)],
        out_specs=(vmem, vmem),
        scratch_shapes=[
            pltpu.VMEM((level_count, tile, width), delay.dtype),
            pltpu.VMEM((level_count, tile // 8, 8, width), f32),
            pltpu.VMEM((level_count + 1, GROUPS, side, gscen, sp), f32),
            pltpu.VMEM((*lg, ratio * side, gscen, sp), f32),
            pltpu.VMEM((*lg, ratio * side, gscen, sp), f32),
            pltpu.VMEM((*lg, side, gscen, sp), f32),
            pltpu.VMEM((*lg, rows, gscen, sp), f32),
            pltpu.VMEM((*lg, gscen, sp), f32),
            pltpu.VMEM((GROUPS, gscen, LANES), f32),
            pltpu.VMEM((cols, 1, LANES), f32),
            pltpu.VMEM((rows, 1, LANES), f32),
            dma((level_count,)),
            dma(lg), dma(lg),
            dma(lg), dma(lg),
            dma(lg), dma((*lg, side)),
            dma((cols,)), dma((cols,)),
            dma((rows,)), dma((rows,)),
        ],
        compiler_params=pltpu.CompilerParams(collective_id=0, has_side_effects=True, vmem_limit_bytes=60 * 1024 * 1024),
    )(arrival, delay, occupancy)
    return times, worst[0, :scenarios]


def solution(mesh):
    side = 1
    while side * side < mesh.shape["row"]:
        side += 1
    placed = (P(None, "col"), P(None, "col", "row"), P())
    return jax.shard_map(
        functools.partial(shards, side), mesh=mesh, in_specs=placed, out_specs=(P(None, "col"), P()), check_vma=False
    )
```

```python
import functools

import jax
import jax.numpy as jnp
from jax import lax
from jax.experimental import pallas as pl
from jax.experimental.pallas import tpu as pltpu
from jax.sharding import PartitionSpec as P

MESH = pl.DeviceIdType.MESH
LANES = 128
GROUPS = 8
LOW = -1000000000.0


def kernel(
    rows, cols, arrival_hbm, delay_hbm, occ_hbm, out_hbm, worst_ref,
    occ_ref, delay_ref, wide_ref, times_ref, part_ref, near_ref, comb_ref, far_ref, fin_ref, crest_ref, peak_ref, top_ref,
    start_sem, occ_sem, load_sem, out_sem, near_send, near_recv, far_send, far_recv, times_send, times_recv, peak_send, peak_recv, top_send, top_recv,
):
    level_count, tile, width = delay_hbm.shape
    groups, side, gscen, sp = times_ref.shape[1:]
    ratio = cols // rows
    row = lax.axis_index("row")
    col = lax.axis_index("col")
    x = row // side
    y = row % side
    z = col // ratio
    p = col % ratio
    keeper = z % side == y
    last = level_count - 1

    def turn(value, n, size):
        return lax.rem(value + n, size)

    barrier = pltpu.get_barrier_semaphore()

    def greet(to_row, to_col):
        pl.semaphore_signal(barrier, inc=1, device_id=(to_row, to_col), device_id_type=MESH)

    for n in range(1, cols):
        greet(row, turn(col, n, cols))
    for n in range(1, rows):
        greet(turn(row, n, rows), col)
    for i in range(1, side):
        for c in range(1, ratio):
            greet(turn(x, i, side) * side + y, z * ratio + turn(p, c, ratio))
    peers = cols - 1 + rows - 1 + (side - 1) * (ratio - 1)

    def load(level, k):
        at = pl.ds(k * sp, sp)
        return pltpu.make_async_copy(delay_hbm.at[level, at], delay_ref.at[level, at], load_sem.at[level, k])

    def arrive(k):
        return pltpu.make_async_copy(arrival_hbm.at[:, :, pl.ds(k * sp, sp)], times_ref.at[0, :, k], start_sem.at[k])

    flags = pltpu.make_async_copy(occ_hbm, occ_ref, occ_sem)

    def widen(level, k):
        def step(i, carry):
            at = pl.ds(pl.multiple_of(k * sp + i * 64, 64), 64)
            wide_ref[level, pl.ds(k * (sp // 8) + i * 8, 8)] = delay_ref[level, at, :].astype(jnp.float32).reshape(8, 8, width)
            return carry

        lax.fori_loop(0, sp // 64, step, 0)

    for k in range(side):
        load(0, k).start()
    for k in range(side):
        arrive(k).start()
    flags.start()
    for level in range(1, level_count):
        for k in range(side):
            load(level, k).start()
    for k in range(side):
        load(0, k).wait()
        widen(0, k)
    for k in range(side):
        arrive(k).wait()
    flags.wait()

    def near_copy(level, g, i, c):
        to_x = turn(x, i, side)
        to_p = turn(p, c, ratio)
        return pltpu.make_async_remote_copy(
            src_ref=part_ref.at[level, g, to_p * side + to_x], dst_ref=near_ref.at[level, g, i * ratio + c],
            send_sem=near_send.at[level, g], recv_sem=near_recv.at[level, g, i],
            device_id=(to_x * side + y, z * ratio + to_p), device_id_type=MESH)

    def near_some(level, g, i, count):
        some = near_ref.at[level, g, pl.ds(1, count)]
        return pltpu.make_async_remote_copy(
            src_ref=some, dst_ref=some, send_sem=near_send.at[level, g], recv_sem=near_recv.at[level, g, i],
            device_id=(turn(x, 1, side) * side + y, col), device_id_type=MESH)

    def spot(i):
        return turn(x, side - i, side) * side + y

    def far_copy(level, g, i):
        return pltpu.make_async_remote_copy(
            src_ref=comb_ref.at[level, g, i], dst_ref=far_ref.at[level, g, turn(z, rows - spot(i), rows)],
            send_sem=far_send.at[level, g], recv_sem=far_recv.at[level, g],
            device_id=(row, spot(i) * ratio + p), device_id_type=MESH)

    def far_all(level, g, count):
        some = far_ref.at[level, g, pl.ds(1, count)]
        return pltpu.make_async_remote_copy(
            src_ref=some, dst_ref=some, send_sem=far_send.at[level, g], recv_sem=far_recv.at[level, g],
            device_id=(row, turn(z, 1, rows) * ratio + p), device_id_type=MESH)

    steps = sorted(
        ((a, b) for a in range(side) for b in range(side) if a or b),
        key=lambda s: -(min(s[0], side - s[0]) + min(s[1], side - s[1])))

    def times_copy(level, g, a, b, k):
        return pltpu.make_async_remote_copy(
            src_ref=fin_ref.at[level, g], dst_ref=times_ref.at[level + 1, g, k],
            send_sem=times_send.at[level, g], recv_sem=times_recv.at[level, g, k],
            device_id=(turn(x, a, side) * side + turn(y, b, side), col), device_id_type=MESH)

    def times_all(level, g):
        some = far_ref.at[level, g, pl.ds(1, rows - 1)]
        return pltpu.make_async_remote_copy(
            src_ref=some, dst_ref=some, send_sem=times_send.at[level, g], recv_sem=times_recv.at[level, g, 0],
            device_id=(turn(row, 1, rows), col), device_id_type=MESH)

    def wait_times(level, g, k):
        @pl.when(jnp.logical_not(jnp.logical_and(keeper, k == x)))
        def _():
            times_copy(level, g, 0, 1, k).wait_recv()

    def compute(level, g):
        def step(n, best):
            @pl.when(jnp.logical_and(jnp.logical_and(level == 0, g == 0), n == side - 1))
            def _():
                pl.semaphore_wait(barrier, peers)

            @pl.when(n == 0)
            def _():
                @pl.when(jnp.logical_and(level > 0, g == 0))
                def _():
                    combine(level - 1, groups - 1)

                @pl.when(jnp.logical_and(level > 0, g < 3))
                def _():
                    finish(level - 1, g + 2)

            @pl.when(n == side - 1)
            def _():
                @pl.when(jnp.logical_and(level > 0, jnp.logical_and(g >= 2, g <= 4)))
                def _():
                    finish(level - 1, g + 3)

                @pl.when(g >= 3)
                def _():
                    combine(level, g - 3)

            k = turn(x, jnp.where(n < 2, n, side + 1 - n), side)

            @pl.when(level > 0)
            def _():
                wait_times(level - 1, g, k)

            value = times_ref[level, g, k]
            for i in range(sp):
                spread = jnp.broadcast_to(value[:, i:i + 1], (gscen, LANES))
                best = tuple(jnp.maximum(b, spread + wide_ref[level, k * (sp // 8) + i // 8, i % 8:i % 8 + 1, c * LANES:(c + 1) * LANES]) for c, b in enumerate(best))
            return best

        best = lax.fori_loop(0, side, step, (jnp.full((gscen, LANES), LOW, jnp.float32),) * (width // LANES))
        crest = jnp.full((gscen, LANES), LOW, jnp.float32)
        for q in range(ratio):
            flag = occ_ref[level, col, row * ratio + q]
            for k in range(side):
                piece = jnp.where(flag > 0, best[q * side + k], jnp.float32(LOW))
                part_ref[level, g, q * side + k] = piece
                crest = jnp.maximum(crest, piece)
        crest_ref[g] = crest

        for i in (2, 1, 3, 0):
            for c in range(ratio):
                if i or c:
                    near_copy(level, g, i, c).start()

    def combine(level, g):
        for i in (0, 1, 3, 2):
            near_some(level, g, i, ratio if i else ratio - 1).wait_recv()
            total = near_ref[level, g, i * ratio] if i else part_ref[level, g, p * side + x]
            for c in range(1, ratio):
                total = jnp.maximum(total, near_ref[level, g, i * ratio + c])
            comb_ref[level, g, i] = total

            @pl.when(z != spot(i))
            def _():
                far_copy(level, g, i).start()

            @pl.when(z == spot(i))
            def _():
                far_ref[level, g, 0] = total

    def finish(level, g):
        @pl.when(keeper)
        def _():
            far_all(level, g, rows - 1).wait_recv()
            total = far_ref[level, g, 0]
            for n in range(1, rows):
                total = jnp.maximum(total, far_ref[level, g, n])
            fin_ref[level, g] = total
            for a, b in steps:
                times_copy(level, g, a, b, x).start()
            times_ref[level + 1, g, x] = total

    def settle(level):
        for g in range(groups):
            near_some(level, g, 0, side * ratio - 1).wait_send()

            @pl.when(jnp.logical_not(keeper))
            def _():
                far_all(level, g, side).wait_send()

            @pl.when(keeper)
            def _():
                far_all(level, g, side - 1).wait_send()
                times_all(level, g).wait_send()

    def peak_copy(n):
        return pltpu.make_async_remote_copy(
            src_ref=peak_ref.at[0], dst_ref=peak_ref.at[n], send_sem=peak_send.at[n], recv_sem=peak_recv.at[n],
            device_id=(row, turn(col, n, cols)), device_id_type=MESH)

    def top_copy(n):
        return pltpu.make_async_remote_copy(
            src_ref=top_ref.at[0], dst_ref=top_ref.at[n], send_sem=top_send.at[n], recv_sem=top_recv.at[n],
            device_id=(turn(row, n, rows), col), device_id_type=MESH)

    def peaks():
        lane = lax.broadcasted_iota(jnp.int32, (gscen, LANES), 1)
        line = lax.broadcasted_iota(jnp.int32, (gscen, LANES), 0)
        peak = jnp.full((1, LANES), LOW, jnp.float32)
        for g in range(groups):
            most = jnp.max(crest_ref[g], axis=1, keepdims=True)
            shown = jnp.where(lane == line + g * gscen, most, jnp.float32(LOW))
            peak = jnp.maximum(peak, jnp.max(shown, axis=0, keepdims=True))
        peak_ref[0] = peak
        for n in range(1, cols):
            peak_copy(n).start()

    def one_level(level, carry):
        def one_group(g, carry):
            compute(level, g)
            return carry

        lax.fori_loop(0, groups, one_group, 0)

        @pl.when(level == last)
        def _():
            peaks()

        @pl.when(level < last)
        def _():
            for k in range(side):
                load(level + 1, k).wait()
                widen(level + 1, k)

        combine(level, groups - 3)
        finish(level, 0)
        combine(level, groups - 2)

        @pl.when(level > 0)
        def _():
            settle(level - 1)

        finish(level, 1)
        return carry

    lax.fori_loop(0, level_count, one_level, 0)
    combine(last, groups - 1)
    for g in range(2, groups - 2):
        finish(last, g)
    top = peak_ref[0]
    for n in range(1, cols):
        peak_copy(n).wait_recv()
        top = jnp.maximum(top, peak_ref[n])
    top_ref[0] = top
    for n in range(1, rows):
        top_copy(n).start()
    for g in range(groups - 2, groups):
        finish(last, g)

    def give(g, k):
        return pltpu.make_async_copy(times_ref.at[level_count, g, k], out_hbm.at[g, :, pl.ds(k * sp, sp)], out_sem)

    for g in range(groups):
        for k in range(side):
            wait_times(last, g, k)
            give(g, k).start()
    for n in range(1, rows):
        top_copy(n).wait_recv()
        top = jnp.maximum(top, top_ref[n])
    worst_ref[...] = top
    settle(last)
    pltpu.make_async_copy(arrival_hbm, out_hbm, out_sem).wait()
    for n in range(1, cols):
        peak_copy(n).wait_send()
    for n in range(1, rows):
        top_copy(n).wait_send()


def shards(side, arrival, delay, occupancy):
    rows, cols = lax.axis_size("row"), lax.axis_size("col")
    scenarios, tile = arrival.shape
    level_count, _, width = delay.shape
    ratio = cols // rows
    sp = tile // side
    gscen = scenarios // GROUPS
    vmem = pl.BlockSpec(memory_space=pltpu.VMEM)
    hbm = pl.BlockSpec(memory_space=pltpu.HBM)
    f32 = jnp.float32
    dma = pltpu.SemaphoreType.DMA
    lg = (level_count, GROUPS)
    times, worst = pl.pallas_call(
        functools.partial(kernel, rows, cols),
        out_shape=(
            jax.ShapeDtypeStruct((GROUPS, gscen, tile), f32),
            jax.ShapeDtypeStruct((1, LANES), f32),
        ),
        in_specs=[hbm, hbm, hbm],
        out_specs=(hbm, vmem),
        scratch_shapes=[
            pltpu.SMEM(occupancy.shape, occupancy.dtype),
            pltpu.VMEM((level_count, tile, width), delay.dtype),
            pltpu.VMEM((level_count, tile // 8, 8, width), f32),
            pltpu.VMEM((level_count + 1, GROUPS, side, gscen, sp), f32),
            pltpu.VMEM((*lg, ratio * side, gscen, sp), f32),
            pltpu.VMEM((*lg, ratio * side, gscen, sp), f32),
            pltpu.VMEM((*lg, side, gscen, sp), f32),
            pltpu.VMEM((*lg, rows, gscen, sp), f32),
            pltpu.VMEM((*lg, gscen, sp), f32),
            pltpu.VMEM((GROUPS, gscen, LANES), f32),
            pltpu.VMEM((cols, 1, LANES), f32),
            pltpu.VMEM((rows, 1, LANES), f32),
            dma((side,)), dma, dma((level_count, side)), dma,
            dma(lg), dma((*lg, side)),
            dma(lg), dma(lg),
            dma(lg), dma((*lg, side)),
            dma((cols,)), dma((cols,)),
            dma((rows,)), dma((rows,)),
        ],
        compiler_params=pltpu.CompilerParams(collective_id=0, has_side_effects=True, vmem_limit_bytes=60 * 1024 * 1024),
    )(arrival.reshape(GROUPS, gscen, tile), delay, occupancy)
    return times.reshape(scenarios, tile), worst[0, :scenarios]


def solution(mesh):
    side = 1
    while side * side < mesh.shape["row"]:
        side += 1
    placed = (P(None, "col"), P(None, "col", "row"), P())
    return jax.shard_map(
        functools.partial(shards, side), mesh=mesh, in_specs=placed, out_specs=(P(None, "col"), P()), check_vma=False
    )
```

```python
import functools

import jax
import jax.numpy as jnp
from jax import lax
from jax.experimental import pallas as pl
from jax.experimental.pallas import tpu as pltpu
from jax.sharding import PartitionSpec as P

MESH = pl.DeviceIdType.MESH
LANES = 128
GROUPS = 8
PAIR = 2
HELD = 1
LOW = -1000000000.0


def kernel(
    rows, cols, arrival_hbm, delay_hbm, occ_hbm, out_hbm, worst_ref,
    occ_ref, delay_ref, wide_ref, times_ref, part_ref, near_ref, comb_ref, far_ref, fin_ref, crest_ref, peak_ref, top_ref,
    start_sem, occ_sem, load_sem, out_sem, near_send, near_recv, far_send, far_recv, times_send, times_recv, peak_send, peak_recv, top_send, top_recv,
):
    level_count, tile, width = delay_hbm.shape
    groups, side, gscen, sp = times_ref.shape[1:]
    ratio = cols // rows
    row = lax.axis_index("row")
    col = lax.axis_index("col")
    x = row // side
    y = row % side
    z = col // ratio
    p = col % ratio
    keeper = z % side == y
    last = level_count - 1

    def turn(value, n, size):
        return lax.rem(value + n, size)

    barrier = pltpu.get_barrier_semaphore()

    def greet(to_row, to_col):
        pl.semaphore_signal(barrier, inc=1, device_id=(to_row, to_col), device_id_type=MESH)

    peers = cols - 1 + rows - 1 + (side - 1) * (ratio - 1)

    def load(level, k):
        at = pl.ds(k * sp, sp)
        return pltpu.make_async_copy(delay_hbm.at[level, at], delay_ref.at[level, at], load_sem.at[level, k])

    def arrive(k):
        return pltpu.make_async_copy(arrival_hbm.at[:, :, pl.ds(k * sp, sp)], times_ref.at[0, :, k], start_sem.at[k])

    flags = pltpu.make_async_copy(occ_hbm, occ_ref, occ_sem)

    def widen(level, k):
        def step(i, carry):
            at = pl.ds(pl.multiple_of(k * sp + i * 64, 64), 64)
            wide_ref[level, pl.ds(k * (sp // 8) + i * 8, 8)] = delay_ref[level, at, :].astype(jnp.float32).reshape(8, 8, width)
            return carry

        lax.fori_loop(0, sp // 64, step, 0)

    for k in range(side):
        load(0, k).start()
    for k in range(side):
        arrive(k).start()
    flags.start()
    for level in range(1, level_count):
        for k in range(side):
            load(level, k).start()
    half = rows // 2
    for n in range(half):
        for turned in {half + n, half - n} - {0}:
            for c in range(ratio):
                greet(row, turn(z, turned, rows) * ratio + turn(p, c, ratio))
    for c in range(1, ratio):
        greet(row, z * ratio + turn(p, c, ratio))
    for n in range(1, rows):
        greet(turn(row, n, rows), col)
    for i in range(1, side):
        for c in range(1, ratio):
            greet(turn(x, i, side) * side + y, z * ratio + turn(p, c, ratio))
    flags.wait()

    def near_copy(level, g, i, c):
        to_x = turn(x, i, side)
        to_p = turn(p, c, ratio)
        return pltpu.make_async_remote_copy(
            src_ref=part_ref.at[level, g, to_p * side + to_x], dst_ref=near_ref.at[level, g, i * ratio + c],
            send_sem=near_send.at[level, g], recv_sem=near_recv.at[level, g, i],
            device_id=(to_x * side + y, z * ratio + to_p), device_id_type=MESH)

    def near_some(level, g, i, count):
        some = near_ref.at[level, g, pl.ds(1, count)]
        return pltpu.make_async_remote_copy(
            src_ref=some, dst_ref=some, send_sem=near_send.at[level, g], recv_sem=near_recv.at[level, g, i],
            device_id=(turn(x, 1, side) * side + y, col), device_id_type=MESH)

    def spot(i):
        return turn(x, side - i, side) * side + y

    def far_copy(level, g, i):
        return pltpu.make_async_remote_copy(
            src_ref=comb_ref.at[level, g, i], dst_ref=far_ref.at[level, g, turn(z, rows - spot(i), rows)],
            send_sem=far_send.at[level, g], recv_sem=far_recv.at[level, g],
            device_id=(row, spot(i) * ratio + p), device_id_type=MESH)

    def far_all(level, g, count):
        some = far_ref.at[level, g, pl.ds(1, count)]
        return pltpu.make_async_remote_copy(
            src_ref=some, dst_ref=some, send_sem=far_send.at[level, g], recv_sem=far_recv.at[level, g],
            device_id=(row, turn(z, 1, rows) * ratio + p), device_id_type=MESH)

    steps = sorted(
        ((a, b) for a in range(side) for b in range(side) if a or b),
        key=lambda s: -(min(s[0], side - s[0]) + min(s[1], side - s[1])))

    def times_copy(level, g, a, b, k):
        return pltpu.make_async_remote_copy(
            src_ref=fin_ref.at[level, g], dst_ref=times_ref.at[level + 1, g, k],
            send_sem=times_send.at[level, g], recv_sem=times_recv.at[level, g, k],
            device_id=(turn(x, a, side) * side + turn(y, b, side), col), device_id_type=MESH)

    def times_all(level, g):
        some = far_ref.at[level, g, pl.ds(1, rows - 1)]
        return pltpu.make_async_remote_copy(
            src_ref=some, dst_ref=some, send_sem=times_send.at[level, g], recv_sem=times_recv.at[level, g, 0],
            device_id=(turn(row, 1, rows), col), device_id_type=MESH)

    def wait_times(level, g, k):
        @pl.when(jnp.logical_not(jnp.logical_and(keeper, k == x)))
        def _():
            times_copy(level, g, 0, 1, k).wait_recv()

    def scatter(level, g):
        for i in (2, 1, 3, 0):
            for c in range(ratio):
                if i or c:
                    near_copy(level, g, i, c).start()

    def blank(high):
        return (jnp.full((high, LANES), LOW, jnp.float32),) * (width // LANES)

    def sweep(level, k, value, best):
        for i in range(sp):
            spread = jnp.broadcast_to(value[:, i:i + 1], (value.shape[0], LANES))
            best = tuple(jnp.maximum(b, spread + wide_ref[level, k * (sp // 8) + i // 8, i % 8:i % 8 + 1, c * LANES:(c + 1) * LANES]) for c, b in enumerate(best))
        return best

    def shown(level, best):
        flag = [occ_ref[level, col, row * ratio + q] for q in range(ratio)]
        return [jnp.where(flag[n // side] > 0, b, jnp.float32(LOW)) for n, b in enumerate(best)]

    def begin(h, carry):
        def step(k, best):
            @pl.when(jnp.logical_and(h == HELD, k == side - 1))
            def _():
                pl.semaphore_wait(barrier, peers)

            @pl.when(h == 0)
            def _():
                load(0, k).wait()
                arrive(k).wait()
                widen(0, k)

            @pl.when(h == groups // PAIR - 1)
            def _():
                @pl.when(k == 0)
                def _():
                    for g in range(PAIR):
                        combine(0, g)

                @pl.when(k == side - 1)
                def _():
                    for g in range(PAIR):
                        combine(0, PAIR + g)

            value = times_ref[0, pl.ds(h * PAIR, PAIR), k].reshape(PAIR * gscen, sp)
            return sweep(0, k, value, best)

        pieces = shown(0, lax.fori_loop(0, side, step, blank(PAIR * gscen)))
        for n, piece in enumerate(pieces):
            for j in range(PAIR):
                part_ref[0, h * PAIR + j, n] = piece[j * gscen:(j + 1) * gscen]

        def send(g, carry):
            scatter(0, g)
            return carry

        lax.fori_loop(jnp.where(h == HELD, 0, h * PAIR), jnp.where(h < HELD, h * PAIR, (h + 1) * PAIR), send, 0)
        return carry

    def compute(level, g):
        def step(n, best):
            @pl.when(jnp.logical_and(n == 0, g < groups - 2))
            def _():
                finish(level - 1, g + 2)

            @pl.when(jnp.logical_and(n == side - 1, g >= 3))
            def _():
                combine(level, g - 3)

            k = turn(x, jnp.where(n < 2, n, side + 1 - n), side)
            wait_times(level - 1, g, k)
            return sweep(level, k, times_ref[level, g, k], best)

        pieces = shown(level, lax.fori_loop(0, side, step, blank(gscen)))
        for n, piece in enumerate(pieces):
            part_ref[level, g, n] = piece
        crest_ref[g] = functools.reduce(jnp.maximum, pieces)
        scatter(level, g)

    def combine(level, g):
        for i in (0, 1, 3, 2):
            near_some(level, g, i, ratio if i else ratio - 1).wait_recv()
            total = near_ref[level, g, i * ratio] if i else part_ref[level, g, p * side + x]
            for c in range(1, ratio):
                total = jnp.maximum(total, near_ref[level, g, i * ratio + c])
            comb_ref[level, g, i] = total

            @pl.when(z != spot(i))
            def _():
                far_copy(level, g, i).start()

            @pl.when(z == spot(i))
            def _():
                far_ref[level, g, 0] = total

    def finish(level, g):
        @pl.when(keeper)
        def _():
            far_all(level, g, rows - 1).wait_recv()
            total = far_ref[level, g, 0]
            for n in range(1, rows):
                total = jnp.maximum(total, far_ref[level, g, n])
            fin_ref[level, g] = total
            for a, b in steps:
                times_copy(level, g, a, b, x).start()
            times_ref[level + 1, g, x] = total

    def settle(level):
        for g in range(groups):
            near_some(level, g, 0, side * ratio - 1).wait_send()

            @pl.when(jnp.logical_not(keeper))
            def _():
                far_all(level, g, side).wait_send()

            @pl.when(keeper)
            def _():
                far_all(level, g, side - 1).wait_send()
                times_all(level, g).wait_send()

    def peak_copy(n):
        return pltpu.make_async_remote_copy(
            src_ref=peak_ref.at[0], dst_ref=peak_ref.at[n], send_sem=peak_send.at[n], recv_sem=peak_recv.at[n],
            device_id=(row, turn(col, n, cols)), device_id_type=MESH)

    def top_copy(n):
        return pltpu.make_async_remote_copy(
            src_ref=top_ref.at[0], dst_ref=top_ref.at[n], send_sem=top_send.at[n], recv_sem=top_recv.at[n],
            device_id=(turn(row, n, rows), col), device_id_type=MESH)

    def peaks():
        lane = lax.broadcasted_iota(jnp.int32, (gscen, LANES), 1)
        line = lax.broadcasted_iota(jnp.int32, (gscen, LANES), 0)
        peak = jnp.full((1, LANES), LOW, jnp.float32)
        for g in range(groups):
            most = jnp.max(crest_ref[g], axis=1, keepdims=True)
            placed = jnp.where(lane == line + g * gscen, most, jnp.float32(LOW))
            peak = jnp.maximum(peak, jnp.max(placed, axis=0, keepdims=True))
        peak_ref[0] = peak
        for n in range(1, cols):
            peak_copy(n).start()

    def ready(level):
        for k in range(side):
            load(level, k).wait()
            widen(level, k)

    def one_level(level, carry):
        def one_group(g, carry):
            compute(level, g)
            return carry

        lax.fori_loop(0, groups, one_group, 0)
        pl.when(level == last)(peaks)
        combine(level, 5)
        finish(level, 0)
        combine(level, 6)

        @pl.when(level < last)
        def _():
            ready(level + 1)

        finish(level, 1)
        combine(level, 7)
        settle(level - 1)
        return carry

    lax.fori_loop(0, groups // PAIR, begin, 0)
    combine(0, 4)
    combine(0, 5)
    finish(0, 0)
    combine(0, 6)
    ready(1)
    finish(0, 1)
    combine(0, 7)
    lax.fori_loop(1, level_count, one_level, 0)
    for g in range(2, groups - 2):
        finish(last, g)
    top = peak_ref[0]
    for n in range(1, cols):
        peak_copy(n).wait_recv()
        top = jnp.maximum(top, peak_ref[n])
    top_ref[0] = top
    for n in range(1, rows):
        top_copy(n).start()
    for g in range(groups - 2, groups):
        finish(last, g)

    def give(g, k):
        return pltpu.make_async_copy(times_ref.at[level_count, g, k], out_hbm.at[g, :, pl.ds(k * sp, sp)], out_sem)

    for g in range(groups):
        for k in range(side):
            wait_times(last, g, k)
            give(g, k).start()
    for n in range(1, rows):
        top_copy(n).wait_recv()
        top = jnp.maximum(top, top_ref[n])
    worst_ref[...] = top
    settle(last)
    pltpu.make_async_copy(arrival_hbm, out_hbm, out_sem).wait()
    for n in range(1, cols):
        peak_copy(n).wait_send()
    for n in range(1, rows):
        top_copy(n).wait_send()


def shards(side, arrival, delay, occupancy):
    rows, cols = lax.axis_size("row"), lax.axis_size("col")
    scenarios, tile = arrival.shape
    level_count, _, width = delay.shape
    ratio = cols // rows
    sp = tile // side
    gscen = scenarios // GROUPS
    vmem = pl.BlockSpec(memory_space=pltpu.VMEM)
    hbm = pl.BlockSpec(memory_space=pltpu.HBM)
    f32 = jnp.float32
    dma = pltpu.SemaphoreType.DMA
    lg = (level_count, GROUPS)
    times, worst = pl.pallas_call(
        functools.partial(kernel, rows, cols),
        out_shape=(
            jax.ShapeDtypeStruct((GROUPS, gscen, tile), f32),
            jax.ShapeDtypeStruct((1, LANES), f32),
        ),
        in_specs=[hbm, hbm, hbm],
        out_specs=(pl.BlockSpec(memory_space=pl.ANY), vmem),
        scratch_shapes=[
            pltpu.SMEM(occupancy.shape, occupancy.dtype),
            pltpu.VMEM((level_count, tile, width), delay.dtype),
            pltpu.VMEM((level_count, tile // 8, 8, width), f32),
            pltpu.VMEM((level_count + 1, GROUPS, side, gscen, sp), f32),
            pltpu.VMEM((*lg, ratio * side, gscen, sp), f32),
            pltpu.VMEM((*lg, ratio * side, gscen, sp), f32),
            pltpu.VMEM((*lg, side, gscen, sp), f32),
            pltpu.VMEM((*lg, rows, gscen, sp), f32),
            pltpu.VMEM((*lg, gscen, sp), f32),
            pltpu.VMEM((GROUPS, gscen, LANES), f32),
            pltpu.VMEM((cols, 1, LANES), f32),
            pltpu.VMEM((rows, 1, LANES), f32),
            dma((side,)), dma, dma((level_count, side)), dma,
            dma(lg), dma((*lg, side)),
            dma(lg), dma(lg),
            dma(lg), dma((*lg, side)),
            dma((cols,)), dma((cols,)),
            dma((rows,)), dma((rows,)),
        ],
        compiler_params=pltpu.CompilerParams(collective_id=0, has_side_effects=True, vmem_limit_bytes=40 * 1024 * 1024),
    )(*(pltpu.with_memory_space_constraint(v, pltpu.HBM) for v in (arrival.reshape(GROUPS, gscen, tile), delay, occupancy)))
    return times.reshape(scenarios, tile), worst[0, :scenarios]


def solution(mesh):
    side = 1
    while side * side < mesh.shape["row"]:
        side += 1
    placed = (P(None, "col"), P(None, "col", "row"), P())
    return jax.shard_map(
        functools.partial(shards, side), mesh=mesh, in_specs=placed, out_specs=(P(None, "col"), P()), check_vma=False
    )
```

```python
import functools

import jax
import jax.numpy as jnp
from jax import lax
from jax.experimental import pallas as pl
from jax.experimental.pallas import tpu as pltpu
from jax.sharding import PartitionSpec as P

MESH = pl.DeviceIdType.MESH
LANES = 128
GROUPS = 8
PAIR = 2
HELD = 1
LOW = -1000000000.0


def kernel(
    rows, cols, arrival_hbm, delay_hbm, occ_hbm, out_hbm, worst_ref,
    occ_ref, delay_ref, wide_ref, times_ref, part_ref, near_ref, comb_ref, far_ref, fin_ref, crest_ref, peak_ref, top_ref,
    start_sem, occ_sem, load_sem, out_sem, near_send, near_recv, far_send, far_recv, times_send, times_recv, peak_send, peak_recv, top_send, top_recv,
):
    level_count, tile, width = delay_hbm.shape
    groups, side, gscen, sp = times_ref.shape[1:]
    ratio = cols // rows
    row = lax.axis_index("row")
    col = lax.axis_index("col")
    x = row // side
    y = row % side
    z = col // ratio
    p = col % ratio
    keeper = z % side == y
    last = level_count - 1

    def turn(value, n, size):
        return lax.rem(value + n, size)

    barrier = pltpu.get_barrier_semaphore()

    def greet(to_row, to_col):
        pl.semaphore_signal(barrier, inc=1, device_id=(to_row, to_col), device_id_type=MESH)

    peers = cols - 1 + rows - 1 + (side - 1) * (ratio - 1)

    def load(level, k):
        at = pl.ds(k * sp, sp)
        return pltpu.make_async_copy(delay_hbm.at[level, at], delay_ref.at[level, at], load_sem.at[level, k])

    def arrive(k):
        return pltpu.make_async_copy(arrival_hbm.at[:, :, pl.ds(k * sp, sp)], times_ref.at[0, :, k], start_sem.at[k])

    flags = pltpu.make_async_copy(occ_hbm, occ_ref, occ_sem)

    def widen(level, k):
        def step(i, carry):
            at = pl.ds(pl.multiple_of(k * sp + i * 64, 64), 64)
            wide_ref[level, pl.ds(k * (sp // 8) + i * 8, 8)] = delay_ref[level, at, :].astype(jnp.float32).reshape(8, 8, width)
            return carry

        lax.fori_loop(0, sp // 64, step, 0)

    for k in range(side):
        load(0, k).start()
    for k in range(side):
        arrive(k).start()
    flags.start()
    for level in range(1, level_count):
        for k in range(side):
            load(level, k).start()
    half = rows // 2
    for n in range(half):
        for turned in {half + n, half - n} - {0}:
            for c in range(ratio):
                greet(row, turn(z, turned, rows) * ratio + turn(p, c, ratio))
    for c in range(1, ratio):
        greet(row, z * ratio + turn(p, c, ratio))
    for n in range(1, rows):
        greet(turn(row, n, rows), col)
    for i in range(1, side):
        for c in range(1, ratio):
            greet(turn(x, i, side) * side + y, z * ratio + turn(p, c, ratio))
    flags.wait()

    def near_copy(level, g, i, c):
        to_x = turn(x, i, side)
        to_p = turn(p, c, ratio)
        return pltpu.make_async_remote_copy(
            src_ref=part_ref.at[level, g, to_p * side + to_x], dst_ref=near_ref.at[level, g, i * ratio + c],
            send_sem=near_send.at[level, g], recv_sem=near_recv.at[level, g, i],
            device_id=(to_x * side + y, z * ratio + to_p), device_id_type=MESH)

    def near_some(level, g, i, count):
        some = near_ref.at[level, g, pl.ds(1, count)]
        return pltpu.make_async_remote_copy(
            src_ref=some, dst_ref=some, send_sem=near_send.at[level, g], recv_sem=near_recv.at[level, g, i],
            device_id=(turn(x, 1, side) * side + y, col), device_id_type=MESH)

    def spot(i):
        return turn(x, side - i, side) * side + y

    def far_copy(level, g, i):
        return pltpu.make_async_remote_copy(
            src_ref=comb_ref.at[level, g, i], dst_ref=far_ref.at[level, g, turn(z, rows - spot(i), rows)],
            send_sem=far_send.at[level, g], recv_sem=far_recv.at[level, g],
            device_id=(row, spot(i) * ratio + p), device_id_type=MESH)

    def far_all(level, g, count):
        some = far_ref.at[level, g, pl.ds(1, count)]
        return pltpu.make_async_remote_copy(
            src_ref=some, dst_ref=some, send_sem=far_send.at[level, g], recv_sem=far_recv.at[level, g],
            device_id=(row, turn(z, 1, rows) * ratio + p), device_id_type=MESH)

    steps = sorted(
        ((a, b) for a in range(side) for b in range(side) if a or b),
        key=lambda s: -(min(s[0], side - s[0]) + min(s[1], side - s[1])))

    def times_copy(level, g, a, b, k):
        return pltpu.make_async_remote_copy(
            src_ref=fin_ref.at[level, g], dst_ref=times_ref.at[level + 1, g, k],
            send_sem=times_send.at[level, g], recv_sem=times_recv.at[level, g, k],
            device_id=(turn(x, a, side) * side + turn(y, b, side), col), device_id_type=MESH)

    def times_all(level, g):
        some = far_ref.at[level, g, pl.ds(1, rows - 1)]
        return pltpu.make_async_remote_copy(
            src_ref=some, dst_ref=some, send_sem=times_send.at[level, g], recv_sem=times_recv.at[level, g, 0],
            device_id=(turn(row, 1, rows), col), device_id_type=MESH)

    def wait_times(level, g, k):
        times_copy(level, g, 0, 1, k).wait_recv()

    def scatter(level, g):
        for i in (2, 1, 3, 0):
            for c in range(ratio):
                if i or c:
                    near_copy(level, g, i, c).start()

    def blank(high):
        return (jnp.full((high, LANES), LOW, jnp.float32),) * (width // LANES)

    def sweep(level, k, value, best):
        for i in range(sp):
            spread = jnp.broadcast_to(value[:, i:i + 1], (value.shape[0], LANES))
            best = tuple(jnp.maximum(b, spread + wide_ref[level, k * (sp // 8) + i // 8, i % 8:i % 8 + 1, c * LANES:(c + 1) * LANES]) for c, b in enumerate(best))
        return best

    def shown(level, best):
        flag = [occ_ref[level, col, row * ratio + q] for q in range(ratio)]
        return [jnp.where(flag[n // side] > 0, b, jnp.float32(LOW)) for n, b in enumerate(best)]

    def begin(h, carry):
        def step(k, best):
            @pl.when(jnp.logical_and(h == HELD, k == side - 1))
            def _():
                pl.semaphore_wait(barrier, peers)

            @pl.when(h == 0)
            def _():
                load(0, k).wait()
                arrive(k).wait()
                widen(0, k)

            @pl.when(h == groups // PAIR - 1)
            def _():
                @pl.when(k == 0)
                def _():
                    for g in range(PAIR):
                        combine(0, g)

                @pl.when(k == side - 1)
                def _():
                    for g in range(PAIR):
                        combine(0, PAIR + g)

            value = times_ref[0, pl.ds(h * PAIR, PAIR), k].reshape(PAIR * gscen, sp)
            return sweep(0, k, value, best)

        pieces = shown(0, lax.fori_loop(0, side, step, blank(PAIR * gscen)))
        for n, piece in enumerate(pieces):
            for j in range(PAIR):
                part_ref[0, h * PAIR + j, n] = piece[j * gscen:(j + 1) * gscen]

        def send(g, carry):
            scatter(0, g)
            return carry

        lax.fori_loop(jnp.where(h == HELD, 0, h * PAIR), jnp.where(h < HELD, h * PAIR, (h + 1) * PAIR), send, 0)
        return carry

    def compute(level, g):
        def step(n, best):
            @pl.when(jnp.logical_and(n == 0, g < groups - 2))
            def _():
                finish(level - 1, g + 2)

            @pl.when(jnp.logical_and(n == 1, g >= 3))
            def _():
                combine(level, g - 3)

            for off in ((side - 1) * n, 1 + n):
                k = turn(x, off, side)
                wait_times(level - 1, g, k)
                best = sweep(level, k, times_ref[level, g, k], best)
            return best

        pieces = shown(level, lax.fori_loop(0, side // 2, step, blank(gscen)))
        for n, piece in enumerate(pieces):
            part_ref[level, g, n] = piece
        crest_ref[g] = functools.reduce(jnp.maximum, pieces)
        scatter(level, g)

    def combine(level, g):
        for i in (0, 1, 3, 2):
            near_some(level, g, i, ratio if i else ratio - 1).wait_recv()
            total = near_ref[level, g, i * ratio] if i else part_ref[level, g, p * side + x]
            for c in range(1, ratio):
                total = jnp.maximum(total, near_ref[level, g, i * ratio + c])
            comb_ref[level, g, i] = total

            @pl.when(z != spot(i))
            def _():
                far_copy(level, g, i).start()

            @pl.when(z == spot(i))
            def _():
                far_ref[level, g, 0] = total

    def finish(level, g):
        @pl.when(keeper)
        def _():
            far_all(level, g, rows - 1).wait_recv()
            total = far_ref[level, g, 0]
            for n in range(1, rows):
                total = jnp.maximum(total, far_ref[level, g, n])
            fin_ref[level, g] = total
            for a, b in steps:
                times_copy(level, g, a, b, x).start()
            pltpu.make_async_copy(fin_ref.at[level, g], times_ref.at[level + 1, g, x], times_recv.at[level, g, x]).start()

    def settle(level):
        for g in range(groups):
            near_some(level, g, 0, side * ratio - 1).wait_send()

            @pl.when(jnp.logical_not(keeper))
            def _():
                far_all(level, g, side).wait_send()

            @pl.when(keeper)
            def _():
                far_all(level, g, side - 1).wait_send()
                times_all(level, g).wait_send()

    def peak_copy(n):
        return pltpu.make_async_remote_copy(
            src_ref=peak_ref.at[0], dst_ref=peak_ref.at[n], send_sem=peak_send.at[n], recv_sem=peak_recv.at[n],
            device_id=(row, turn(col, n, cols)), device_id_type=MESH)

    def top_copy(n):
        return pltpu.make_async_remote_copy(
            src_ref=top_ref.at[0], dst_ref=top_ref.at[n], send_sem=top_send.at[n], recv_sem=top_recv.at[n],
            device_id=(turn(row, n, rows), col), device_id_type=MESH)

    def peaks():
        lane = lax.broadcasted_iota(jnp.int32, (gscen, LANES), 1)
        line = lax.broadcasted_iota(jnp.int32, (gscen, LANES), 0)
        peak = jnp.full((1, LANES), LOW, jnp.float32)
        for g in range(groups):
            most = jnp.max(crest_ref[g], axis=1, keepdims=True)
            placed = jnp.where(lane == line + g * gscen, most, jnp.float32(LOW))
            peak = jnp.maximum(peak, jnp.max(placed, axis=0, keepdims=True))
        peak_ref[0] = peak
        for n in range(1, cols):
            peak_copy(n).start()

    def ready(level):
        for k in range(side):
            load(level, k).wait()
            widen(level, k)

    def one_level(level, carry):
        def one_group(g, carry):
            compute(level, g)
            return carry

        lax.fori_loop(0, groups, one_group, 0)
        pl.when(level == last)(peaks)
        combine(level, 5)
        finish(level, 0)
        combine(level, 6)

        @pl.when(level < last)
        def _():
            ready(level + 1)

        finish(level, 1)
        combine(level, 7)
        settle(level - 1)
        return carry

    lax.fori_loop(0, groups // PAIR, begin, 0)
    combine(0, 4)
    combine(0, 5)
    finish(0, 0)
    combine(0, 6)
    ready(1)
    finish(0, 1)
    combine(0, 7)
    lax.fori_loop(1, level_count, one_level, 0)
    for g in range(2, groups - 2):
        finish(last, g)
    top = peak_ref[0]
    for n in range(1, cols):
        peak_copy(n).wait_recv()
        top = jnp.maximum(top, peak_ref[n])
    top_ref[0] = top
    for n in range(1, rows):
        top_copy(n).start()
    for g in range(groups - 2, groups):
        finish(last, g)

    def give(g, k):
        return pltpu.make_async_copy(times_ref.at[level_count, g, k], out_hbm.at[g, :, pl.ds(k * sp, sp)], out_sem)

    for g in range(groups):
        for k in range(side):
            wait_times(last, g, k)
            give(g, k).start()
    for n in range(1, rows):
        top_copy(n).wait_recv()
        top = jnp.maximum(top, top_ref[n])
    worst_ref[...] = top
    settle(last)
    pltpu.make_async_copy(arrival_hbm, out_hbm, out_sem).wait()
    for n in range(1, cols):
        peak_copy(n).wait_send()
    for n in range(1, rows):
        top_copy(n).wait_send()


def shards(side, arrival, delay, occupancy):
    rows, cols = lax.axis_size("row"), lax.axis_size("col")
    scenarios, tile = arrival.shape
    level_count, _, width = delay.shape
    ratio = cols // rows
    sp = tile // side
    gscen = scenarios // GROUPS
    vmem = pl.BlockSpec(memory_space=pltpu.VMEM)
    hbm = pl.BlockSpec(memory_space=pltpu.HBM)
    f32 = jnp.float32
    dma = pltpu.SemaphoreType.DMA
    lg = (level_count, GROUPS)
    times, worst = pl.pallas_call(
        functools.partial(kernel, rows, cols),
        out_shape=(
            jax.ShapeDtypeStruct((GROUPS, gscen, tile), f32),
            jax.ShapeDtypeStruct((1, LANES), f32),
        ),
        in_specs=[hbm, hbm, hbm],
        out_specs=(pl.BlockSpec(memory_space=pl.ANY), vmem),
        scratch_shapes=[
            pltpu.SMEM(occupancy.shape, occupancy.dtype),
            pltpu.VMEM((level_count, tile, width), delay.dtype),
            pltpu.VMEM((level_count, tile // 8, 8, width), f32),
            pltpu.VMEM((level_count + 1, GROUPS, side, gscen, sp), f32),
            pltpu.VMEM((*lg, ratio * side, gscen, sp), f32),
            pltpu.VMEM((*lg, ratio * side, gscen, sp), f32),
            pltpu.VMEM((*lg, side, gscen, sp), f32),
            pltpu.VMEM((*lg, rows, gscen, sp), f32),
            pltpu.VMEM((*lg, gscen, sp), f32),
            pltpu.VMEM((GROUPS, gscen, LANES), f32),
            pltpu.VMEM((cols, 1, LANES), f32),
            pltpu.VMEM((rows, 1, LANES), f32),
            dma((side,)), dma, dma((level_count, side)), dma,
            dma(lg), dma((*lg, side)),
            dma(lg), dma(lg),
            dma(lg), dma((*lg, side)),
            dma((cols,)), dma((cols,)),
            dma((rows,)), dma((rows,)),
        ],
        compiler_params=pltpu.CompilerParams(collective_id=0, has_side_effects=True, vmem_limit_bytes=40 * 1024 * 1024),
    )(*(pltpu.with_memory_space_constraint(v, pltpu.HBM) for v in (arrival.reshape(GROUPS, gscen, tile), delay, occupancy)))
    return times.reshape(scenarios, tile), worst[0, :scenarios]


def solution(mesh):
    side = 1
    while side * side < mesh.shape["row"]:
        side += 1
    placed = (P(None, "col"), P(None, "col", "row"), P())
    return jax.shard_map(
        functools.partial(shards, side), mesh=mesh, in_specs=placed, out_specs=(P(None, "col"), P()), check_vma=False
    )
```
